32 devices in a mesh: groups: 2 (over y), ep: 16 (over z, x, core), node: 1.
Axes of the slice: x: 2, y: 2, z: 4, core: 2. Of those that a mesh axis runs over, the one named last changes fastest.
Arguments:
- queries: bfloat16 [4096, 64, 576], P(('groups', 'ep'), 'node'), parts along dimension 0, may hold values from -16 to 16
- latent_kv: bfloat16 [4096, 576], P(('groups', 'ep')), parts along dimension 0, may hold values from -4 to 4
- w_value: bfloat16 [64, 512, 128], P('node'), may hold values from -0.25 to 0.25
- moe_tokens: bfloat16 [1024, 4096], P(('groups', 'ep')), parts along dimension 0, may hold values from -6 to 6
- routes: int32 [1024, 8], P(('groups', 'ep')), parts along dimension 0, may hold values from 0 to 15, all different within a row; in each aligned block of 32 rows (0 to 31, 32 to 63, ...) at most 24 rows name the same one
- router: bfloat16 [4096, 16], replicated, may hold values from -0.25 to 0.25
- w_gate: bfloat16 [16, 4096, 2048], P('ep', None, 'node'), may hold values from -0.09375 to 0.09375
- w_up: bfloat16 [16, 4096, 2048], P('ep', None, 'node'), may hold values from -0.09375 to 0.09375
- w_down: bfloat16 [16, 2048, 4096], P('ep', 'node'), may hold values from -0.125 to 0.125
Outputs:
- attention_out: bfloat16 [4096, 8192], P(('groups', 'ep'), 'node'), parts along dimension 0
- moe_out: bfloat16 [1024, 4096], P(('groups', 'ep'), 'node'), parts along dimension 0
The draws below stay inside these ranges and needn't reach their ends.
There are 2 independent parts, one for each index of `groups`. The reference program is written for one: setup_inputs(seed, part) draws one part's arguments, and reference() takes and returns one part's arrays. A program takes and returns all parts, laid end to end along the dimension named above; an argument that names none is the same for every part. Nothing has to cross between parts.
Inputs may be any that keep to these rules, and one draw needn't show every extreme that they name: `routes`: each row names 8 different experts; among the 32 rows of one index of ep no expert is named by more than 24 rows, a bound that some block reaches of them.
All inputs are finite; a program needn't handle non-finite values.
Results may differ from the reference program's by a relative error of at most 0.015.
Values may be sent and summed in bfloat16 or wider, within the bound.
A program may use at most 192 MiB of HBM per device.

```python
import math
import jax
import jax.numpy as jnp
import numpy as np
from jax import lax

D = 4096
FF = 2048
HEADS = 64
LATENT = 512
ROPE = 64
VHEAD = 128
TOPK = 8
EXPERTS = 16
SEQ_DEV = 128
SEQ = 2048
TB_DEV = 32
TOKB = 512
CAP = 24
N_EP = 16
N_NODE = 1


def attention_pair(key):
    width = LATENT + ROPE
    latent_key, query_key = jax.random.split(jax.random.fold_in(key, 11), 2)
    latent = jnp.clip(jax.random.normal(latent_key, (SEQ, width), jnp.float32), -4.0, 4.0)
    queries = jnp.clip(jax.random.normal(query_key, (SEQ, HEADS, width), jnp.float32), -4.0, 4.0)
    return (latent, queries)


def draw_queries(key, part):
    return attention_pair(key)[1].astype(jnp.bfloat16)


def draw_latent_kv(key, part):
    return attention_pair(key)[0].astype(jnp.bfloat16)


def shard_levels(stream_key, dims, shards, low, largest):
    loudness = 1.0
    for dim, shards_of in shards:
        draws = jax.random.uniform(jax.random.fold_in(jax.random.fold_in(stream_key, 6), dim), (shards_of,), jnp.float32, low / len(shards), largest / len(shards))
        loudness = loudness * jnp.repeat(jnp.exp(draws), dims[dim] // shards_of).reshape((-1,) + (1,) * (len(dims) - 1 - dim))
    return loudness


def shared_out(own_key, own, number, rows, count, top, limit, lean):
    ranking = jax.random.permutation(own_key, count)
    crowded, usual = portions_of(count, rows * top, limit, lean, True), portions_of(count, rows * top, limit, lean, False)
    places = jnp.arange(count)

    def named(tallies, offset_by):
        used = int((tallies > 0).sum())
        fixed = max(1, used // 4)
        moved = fixed + (places - fixed + offset_by * (used - fixed)) % max(1, count - fixed)
        return jnp.zeros((count,), jnp.int32).at[ranking[jnp.where(places < fixed, places, moved)]].set(jnp.asarray(tallies, jnp.int32))

    tallies = jnp.where(number % 4 == 0, named(crowded, number // 4), named(usual, number - number // 4 - 1))
    mixed = jax.random.permutation(jax.random.fold_in(own, 3), count)
    source_of, receiver = mixed[0:count // 2 * 2:2], mixed[1:count // 2 * 2:2]
    margin = jnp.minimum(tallies[source_of] - 1, limit - tallies[receiver]) // 2
    margin = jnp.where((source_of == ranking[0]) | (receiver == ranking[0]) | (tallies[receiver] == 0), 0, jnp.maximum(margin, 0))
    moved = jax.random.randint(jax.random.fold_in(own, 4), (count // 2,), 0, 1 << 20) % (margin + 1)
    tallies = tallies.at[source_of].add(-moved).at[receiver].add(moved)
    labels = jnp.searchsorted(jnp.cumsum(tallies), jnp.arange(rows * top), side="right").astype(jnp.int32)
    table = labels.reshape(top, rows).T
    table = table[jax.random.permutation(jax.random.fold_in(own, 1), rows)]
    offset_by = jax.random.randint(jax.random.fold_in(own, 2), (rows, 1), 0, top)
    return jnp.take_along_axis(table, (jnp.arange(top)[None, :] + offset_by) % top, axis=1)


def portions_of(count, total, reach, skew, full):
    portions = [(1 << 20) // math.isqrt(grade ** skew) + 1 for grade in range(1, count + 1)]
    largest = reach if full else min(reach, max(-(-total // count), total * portions[0] // sum(portions)))
    least = 1 if total - largest >= count - 1 else 0
    holding, rest = [largest] + [least] * (count - 1), total - largest - least * (count - 1)
    while rest > 0:
        candidates = [i for i in range(1, count) if holding[i] < largest] or [i for i in range(1, count) if holding[i] < reach]
        mass, left = sum([portions[i] for i in candidates]), rest
        for i in candidates:
            extra = min(reach - holding[i], max(1, left * portions[i] // mass), rest)
            holding[i] = holding[i] + extra
            rest = rest - extra
    return np.array(holding)


def centred(rng, extent, scale, reach, cuts=(), held_as=jnp.bfloat16):
    values = jax.random.normal(rng, extent, jnp.float32) * scale
    if len(cuts) > 0:
        values = shard_levels(rng, extent, cuts, -0.22, 0.18) * values
    return jnp.clip(values, min=-reach, max=reach).astype(held_as)


def setup_inputs(seed: int = 0, part: int = 0) -> dict:
    streams_of = jax.random.split(jax.random.key(seed), 10)
    part_keys = jax.random.split(jax.random.fold_in(streams_of[9], part), 10)
    queries = draw_queries(jax.random.fold_in(jax.random.fold_in(streams_of[9], part), 71), part)
    latent_kv = draw_latent_kv(jax.random.fold_in(jax.random.fold_in(streams_of[9], part), 71), part)
    w_value = centred(streams_of[2], (HEADS, LATENT, VHEAD), LATENT ** -0.5, 0.25)
    moe_tokens = centred(part_keys[3], (TOKB, D), 1.0, 6.0, ((0, 16),))
    routes_keys = jax.random.split(jax.random.fold_in(part_keys[4], 1), TOKB // TB_DEV)
    routes_turns = jax.random.permutation(jax.random.fold_in(part_keys[4], 3), TOKB // TB_DEV)
    routes = jax.vmap(lambda own, number: shared_out(jax.random.fold_in(part_keys[4], 2), own, number, TB_DEV, EXPERTS, TOPK, CAP, 1))(routes_keys, routes_turns).reshape((TOKB, TOPK))
    router = centred(streams_of[5], (D, EXPERTS), (D // 9) ** -0.5, 0.25)
    w_gate = centred(streams_of[6], (EXPERTS, D, FF), D ** -0.5, 0.09375, ((0, 16),))
    w_up = centred(streams_of[7], (EXPERTS, D, FF), D ** -0.5, 0.09375, ((0, 16),))
    w_down = centred(streams_of[8], (EXPERTS, FF, D), FF ** -0.5, 0.125, ((0, 16),))
    return {"queries": queries, "latent_kv": latent_kv, "w_value": w_value, "moe_tokens": moe_tokens, "routes": routes, "router": router, "w_gate": w_gate, "w_up": w_up, "w_down": w_down}


ROUTED_SCALE = 2.5


def attend_rows(block, first, latent_kv, w_value):
    width = latent_kv.shape[1]
    latent_width = w_value.shape[1]
    scale = (w_value.shape[2] + width - latent_width) ** -0.5
    scores = jnp.einsum("qhc,kc->qhk", block.astype(jnp.float32), latent_kv.astype(jnp.float32)) * scale
    query_pos = first + jnp.arange(block.shape[0], dtype=jnp.int32)
    key_pos = jnp.arange(latent_kv.shape[0], dtype=jnp.int32)
    visible = key_pos[None, None, :] <= query_pos[:, None, None]
    scores = jnp.where(visible, scores, -1.0e30)
    row_max = jnp.max(scores, axis=2, keepdims=True)
    raised = jnp.where(visible, jnp.exp(scores - row_max), 0.0)
    totals = jnp.sum(raised, axis=2, keepdims=True)
    probs = lax.optimization_barrier(raised.astype(jnp.bfloat16)).astype(jnp.float32)
    values = latent_kv[:, :latent_width].astype(jnp.float32)
    context = jnp.einsum("qhk,kc->qhc", probs, values) / totals
    context = lax.optimization_barrier(context.astype(jnp.bfloat16)).astype(jnp.float32)
    result = jnp.einsum("qhc,hcv->qhv", context, w_value.astype(jnp.float32))
    return result.astype(jnp.bfloat16).reshape(block.shape[0], -1)


def attention_part(queries, latent_kv, w_value):
    blocks = queries.reshape(N_EP, SEQ_DEV, queries.shape[1], queries.shape[2])
    firsts = jnp.arange(N_EP, dtype=jnp.int32) * SEQ_DEV

    def one_block(packed):
        return attend_rows(packed[0], packed[1], latent_kv, w_value)

    outputs = lax.map(one_block, (blocks, firsts))
    return outputs.reshape(queries.shape[0], -1)


def moe_part(moe_tokens, routes, router, w_gate, w_up, w_down):
    tokens_all, top = routes.shape
    experts = router.shape[1]
    logits = jnp.dot(moe_tokens, router, preferred_element_type=jnp.float32)
    affinity = jax.nn.sigmoid(logits)
    chosen = jnp.take_along_axis(affinity, routes, axis=1)
    gates = ROUTED_SCALE * chosen / jnp.sum(chosen, axis=1, keepdims=True)
    blocks = routes.reshape(N_EP, TB_DEV, top)
    expert_range = jnp.arange(experts, dtype=jnp.int32)
    member = jnp.any(blocks[:, :, :, None] == expert_range[None, None, None, :], axis=2).astype(jnp.int32)
    before = jnp.cumsum(member, axis=1) - member
    slots = jnp.take_along_axis(before, blocks, axis=2)
    rows = (jnp.arange(N_EP, dtype=jnp.int32)[:, None, None] * CAP + slots).reshape(-1)
    expert_ids = routes.reshape(-1)
    token_ids = jnp.repeat(jnp.arange(tokens_all, dtype=jnp.int32), top)
    table = jnp.zeros((experts, N_EP * CAP), jnp.int32).at[expert_ids, rows].set(token_ids)
    weights = jnp.zeros((experts, N_EP * CAP), jnp.float32).at[expert_ids, rows].set(gates.reshape(-1))

    def one_expert(total, packed):
        row_ids, row_gates, gate_w, up_w, down_w = packed
        inputs = moe_tokens[row_ids]
        gate = jnp.dot(inputs, gate_w, preferred_element_type=jnp.float32)
        upward = jnp.dot(inputs, up_w, preferred_element_type=jnp.float32)
        hidden = lax.optimization_barrier((jax.nn.silu(gate) * upward).astype(jnp.bfloat16)).astype(jnp.float32)
        pieces = hidden.reshape(row_ids.shape[0], N_NODE, -1)
        downs = down_w.reshape(N_NODE, -1, down_w.shape[1]).astype(jnp.float32)
        partial_value = jnp.einsum("rbf,bfd->rbd", pieces, downs)
        partial_value = lax.optimization_barrier(partial_value.astype(jnp.bfloat16)).astype(jnp.float32)
        summed = jnp.sum(partial_value, axis=1)
        return total.at[row_ids].add(row_gates[:, None] * summed), None

    start = jnp.zeros((tokens_all, moe_tokens.shape[1]), jnp.float32)
    total, ignored = lax.scan(one_expert, start, (table, weights, w_gate, w_up, w_down))
    return total.astype(jnp.bfloat16)


def reference(queries, latent_kv, w_value, moe_tokens, routes, router, w_gate, w_up, w_down):
    attention_out = attention_part(queries, latent_kv, w_value)
    moe_out = moe_part(moe_tokens, routes, router, w_gate, w_up, w_down)
    return (attention_out, moe_out)
```

```python
import functools

import jax
import jax.numpy as jnp
from jax import lax
from jax.experimental import pallas as pl
from jax.experimental.pallas import tpu as pltpu
from jax.sharding import PartitionSpec as P

ROUTED_SCALE = 2.5
NEGATIVE = -1e30
LOG2E = 1.4426950408889634
MESH = pl.DeviceIdType.MESH
F32 = jnp.float32
BF16 = jnp.bfloat16
LANES = 128
UP_SLOTS = 3
DOWN_SLOTS = 3
MOE_AT = 6


def layer_kernel(dims, q_ref, kv_ref, wv_ref, tok_ref, routes_ref, router_ref, wg_ref, wu_ref,
                 wd_ref, out_ref, moe_ref, *scratch):
    (zs, heads, width, latent, vdim, seq_dev, tb, model, ff, experts, cap, scale, ufc, fc) = dims
    (kvt_all, kv_all, q_a, q_b, s_a, s_b, m_a, m_b, l_a, l_b, acc_a, acc_b, wv_a, wv_b, tok_all,
     aux, rows, hidden, chosen_t, gate_col, contrib, recv1, part2, recv2, part3, recv3, wg_buf,
     wu_buf, wd_buf, q_sem, wv_sem, own_sem, kv_send, kv_recv, tok_send, tok_recv, wg_sem, wu_sem,
     wd_sem, s1_send, s1_recv, s2_send, s2_recv, s3_send, s3_recv) = scratch
    me = lax.axis_index("ep")
    z = me // 4
    x = lax.rem(me // 2, 2)
    c = lax.rem(me, 2)
    chunk = 4 * seq_dev
    pairs = heads // 2
    turns = pairs // 2
    moe_at = min(MOE_AT, turns - 1)
    group = 2 * zs * tb
    group_slots = 2 * zs * cap
    up_steps = ff // ufc
    down_steps = model // fc
    factor = scale * LOG2E

    def at(zz, xx, cc):
        return {"ep": zz * 4 + xx * 2 + cc}

    peers = [at(lax.rem(z + d, zs), x, c) for d in range(1, zs)]
    across = at(z, 1 - x, c)
    partner = at(z, x, 1 - c)

    own_kv = pltpu.make_async_copy(
        kv_ref,
        kvt_all.at[z, pl.ds(0, width), pl.ds(pl.multiple_of((x * 2 + c) * seq_dev, seq_dev), seq_dev)],
        own_sem.at[0],
    )
    own_kv.start()

    def block_row(zz, xx):
        return pl.multiple_of((xx * zs + zz) * tb, tb)

    own_tok = pltpu.make_async_copy(
        tok_ref, tok_all.at[c, pl.ds(block_row(z, x), tb), pl.ds(0, model)], own_sem.at[1]
    )
    own_tok.start()

    def q_copies(pair, buf, slot, base):
        return [
            pltpu.make_async_copy(
                q_ref.at[2 * pair + h],
                buf.at[slot, pl.ds(0, width), pl.ds(h * seq_dev, seq_dev)],
                q_sem.at[base, slot, h],
            )
            for h in range(2)
        ]

    def wv_copy(pair, buf, slot, base):
        return pltpu.make_async_copy(
            wv_ref.at[pl.ds(2 * pair, 2)], buf.at[slot], wv_sem.at[base, slot]
        )

    for copy in q_copies(0, q_a, 0, 0) + q_copies(1, q_b, 0, 1):
        copy.start()

    def up_copies(n):
        slot = lax.rem(n, UP_SLOTS)
        cols = pl.ds(pl.multiple_of(n * ufc, ufc), ufc)
        return (
            pltpu.make_async_copy(wg_ref.at[0, :, cols], wg_buf.at[slot], wg_sem.at[slot]),
            pltpu.make_async_copy(wu_ref.at[0, :, cols], wu_buf.at[slot], wu_sem.at[slot]),
        )

    def down_copy(n):
        slot = lax.rem(n, DOWN_SLOTS)
        cols = pl.ds(pl.multiple_of(n * fc, fc), fc)
        return pltpu.make_async_copy(wd_ref.at[0, :, cols], wd_buf.at[slot], wd_sem.at[slot])

    barrier = pltpu.get_barrier_semaphore()
    for peer in peers + [across, partner]:
        pl.semaphore_signal(barrier, inc=1, device_id=peer, device_id_type=MESH)
    pl.semaphore_wait(barrier, zs + 1)

    def kv_block(zz, xx, cc):
        return kvt_all.at[
            zz, pl.ds(0, width), pl.ds(pl.multiple_of((xx * 2 + cc) * seq_dev, seq_dev), seq_dev)
        ]

    def kv_send_to(zz, xx, cc, target, index):
        block = kv_block(zz, xx, cc)
        return pltpu.make_async_remote_copy(
            src_ref=block,
            dst_ref=block,
            send_sem=kv_send.at[index],
            recv_sem=kv_recv.at[zz * 4 + xx * 2 + cc],
            device_id=target,
            device_id_type=MESH,
        )

    def kv_wait(zz, xx, cc):
        kv_send_to(zz, xx, cc, partner, 0).wait_recv()

    def kv_turn(zz, xx, cc):
        cols = pl.ds(pl.multiple_of((xx * 2 + cc) * seq_dev, seq_dev), seq_dev)
        at_row = pl.ds(pl.multiple_of((zz * 4 + xx * 2 + cc) * seq_dev, seq_dev), seq_dev)
        kv_all[at_row, :] = jnp.transpose(kvt_all[zz, :, cols])

    kvt_all[:, width:, :] = jnp.zeros((zs, kvt_all.shape[1] - width, chunk), BF16)
    for buf in (q_a, q_b):
        buf[:, width:, :] = jnp.zeros((2, buf.shape[1] - width, 2 * seq_dev), BF16)
    own_kv.wait()
    kv_send_to(z, x, c, across, zs - 1).start()
    kv_send_to(z, x, c, partner, 2 * zs - 1).start()
    for d in range(1, zs):

        @pl.when(z + d < zs)
        def _():
            kv_send_to(z, x, c, at(z + d, x, c), d - 1).start()

    own_tok.wait()

    own_rows = pl.ds(block_row(z, x), tb)
    logits = lax.dot_general(
        router_ref[...],
        tok_all[c, own_rows, :model],
        (((1,), (1,)), ((), ())),
        preferred_element_type=F32,
    )
    affinity = jax.nn.sigmoid(logits)
    expert_id = lax.broadcasted_iota(jnp.int32, (experts, tb), 0)
    named = jnp.zeros((experts, tb), F32)
    for k in range(routes_ref.shape[0]):
        named = jnp.where(routes_ref[k : k + 1, :] == expert_id, 1.0, named)
    kept = affinity * named
    gates = ROUTED_SCALE * kept / jnp.sum(kept, axis=0, keepdims=True)
    high = gates.astype(BF16).astype(F32)
    aux[...] = jnp.zeros(aux.shape, F32)
    aux[0:experts, 0:tb] = high
    aux[experts : 2 * experts, 0:tb] = gates - high
    aux[2 * experts : 3 * experts, 0:tb] = named
    tok_all[c, own_rows, model:] = jnp.transpose(aux[...])[:tb].astype(BF16)

    def tok_send_to(zz, xx, cc, target, index):
        block = tok_all.at[cc, pl.ds(block_row(zz, xx), tb)]
        return pltpu.make_async_remote_copy(
            src_ref=block,
            dst_ref=block,
            send_sem=tok_send.at[index],
            recv_sem=tok_recv.at[zz * 4 + xx * 2 + cc],
            device_id=target,
            device_id_type=MESH,
        )

    def tok_wait(zz, xx, cc):
        tok_send_to(zz, xx, cc, partner, 0).wait_recv()

    kv_turn(z, x, c)

    for d in range(1, zs):

        @pl.when(z - d >= 0)
        def _():
            kv_wait(z - d, x, c)
            kv_send_to(z - d, x, c, across, zs - 1 + d).start()
            kv_send_to(z - d, x, c, partner, 2 * zs - 1 + d).start()
            kv_turn(z - d, x, c)

    tok_send_to(z, x, c, across, zs - 1).start()
    for d in range(1, zs):
        tok_send_to(z, x, c, peers[d - 1], d - 1).start()
    tok_send_to(z, x, c, partner, 2 * zs - 1).start()

    for n in range(min(UP_SLOTS, up_steps)):
        for copy in up_copies(n):
            copy.start()
    for n in range(min(DOWN_SLOTS, down_steps)):
        down_copy(n).start()

    for d in range(zs):

        @pl.when(z - d >= 0)
        def _():
            kv_wait(z - d, 1 - x, c)
            kv_send_to(z - d, 1 - x, c, partner, 3 * zs - 1 + d).start()
            kv_turn(z - d, 1 - x, c)

    for d in range(zs):
        for xx in (x, 1 - x):

            @pl.when(z - d >= 0)
            def _():
                kv_wait(z - d, xx, 1 - c)
                kv_turn(z - d, xx, 1 - c)

    def scores_of(n, q, s, m, first):
        base = pl.multiple_of(n * chunk, chunk)
        score = jnp.dot(kv_all[pl.ds(base, chunk), :], q, preferred_element_type=F32)
        row = lax.broadcasted_iota(jnp.int32, score.shape, 0)
        col = lax.rem(lax.broadcasted_iota(jnp.int32, score.shape, 1), seq_dev)
        score = jnp.where(row - col <= me * seq_dev - base, score, NEGATIVE)
        s[pl.ds(base, chunk), :] = score
        high8 = jnp.max(score.reshape(chunk // 8, 8, score.shape[1]), axis=0)
        m[...] = high8 if first else jnp.maximum(m[...], high8)

    def values_of(n, s, m, l, acc, first):
        base = pl.multiple_of(n * chunk, chunk)
        top = jnp.max(m[...], axis=0, keepdims=True) * factor
        raised = jnp.exp2(s[pl.ds(base, chunk), :] * factor - top)
        sums = jnp.sum(raised.reshape(chunk // 8, 8, raised.shape[1]), axis=0)
        value = jnp.dot(kvt_all[n, :latent, :], raised.astype(BF16), preferred_element_type=F32)
        if first:
            l[...] = sums
            acc[...] = value
        else:
            l[...] += sums
            acc[...] += value

    def finish(pair, l, acc, wv, slot):
        totals = jnp.sum(l[...], axis=0, keepdims=True)
        context = (acc[...] * (1.0 / totals)).astype(BF16)
        for h in range(2):
            value = lax.dot_general(
                context[:, h * seq_dev : (h + 1) * seq_dev],
                wv[slot, h],
                (((0,), (0,)), ((), ())),
                preferred_element_type=F32,
            )
            cols = pl.ds(pl.multiple_of((2 * pair + h) * vdim, vdim), vdim)
            out_ref[:, cols] = value.astype(BF16)

    set_a = (q_a, s_a, m_a, l_a, acc_a, wv_a, 0)
    set_b = (q_b, s_b, m_b, l_b, acc_b, wv_b, 1)

    def half(i, cur, prev):
        q, s, m, l, acc, wv, parity = cur
        _, s_p, m_p, l_p, acc_p, _, _ = prev
        pair = 2 * i + parity
        slot = lax.rem(i, 2)
        other = 1 - slot
        for copy in q_copies(pair, q, slot, parity):
            copy.wait()

        @pl.when(i + 1 < turns)
        def _():
            for copy in q_copies(pair + 2, q, other, parity):
                copy.start()

        @pl.when(i >= 1)
        def _():
            wv_copy(pair - 2, wv, other, parity).wait()

        wv_copy(pair, wv, slot, parity).start()
        scores_of(0, q[slot], s, m, True)
        values_of(0, s_p, m_p, l_p, acc_p, True)
        finish(jnp.maximum(pair - 2, 0), l, acc, wv, other)

        def more(n, carry):
            scores_of(n, q[slot], s, m, False)
            values_of(n, s_p, m_p, l_p, acc_p, False)
            return carry

        lax.fori_loop(1, z + 1, more, 0)

    def from_peer(d):
        zz = lax.rem(z + d, zs)
        tok_wait(zz, x, c)
        tok_send_to(zz, x, c, across, zs - 1 + d).start()
        tok_send_to(zz, x, c, partner, 2 * zs - 1 + d).start()

    def from_across(d):
        zz = lax.rem(z + d, zs)
        tok_wait(zz, 1 - x, c)
        tok_send_to(zz, 1 - x, c, partner, 3 * zs - 1 + d).start()

    def from_partner():
        for d in range(zs):
            for xx in (x, 1 - x):
                tok_wait(lax.rem(z + d, zs), xx, 1 - c)

    gather_steps = [functools.partial(from_across, 0)]
    gather_steps += [functools.partial(from_peer, d) for d in range(1, zs)]
    gather_steps += [functools.partial(from_across, d) for d in range(1, zs)]
    gather_steps += [from_partner]
    spots = [
        (2 * moe_at * (a + 1)) // len(gather_steps) for a in range(len(gather_steps))
    ]

    def features(k):
        return pl.ds(pl.multiple_of(k * fc, fc), fc)

    half_rows = group // 2

    def first_copy(k):
        return pltpu.make_async_remote_copy(
            src_ref=contrib.at[1 - c, :, features(k)],
            dst_ref=recv1.at[:, features(k)],
            send_sem=s1_send.at[k],
            recv_sem=s1_recv.at[k],
            device_id=partner,
            device_id_type=MESH,
        )

    def second_copy(k):
        away = pl.ds(pl.multiple_of((1 - x) * half_rows, half_rows), half_rows)
        return pltpu.make_async_remote_copy(
            src_ref=part2.at[away, features(k)],
            dst_ref=recv2.at[:, features(k)],
            send_sem=s2_send.at[k],
            recv_sem=s2_recv.at[k],
            device_id=across,
            device_id_type=MESH,
        )

    def third_copy(k, d):
        to = lax.rem(z + d, zs)
        return pltpu.make_async_remote_copy(
            src_ref=part3.at[pl.ds(pl.multiple_of(to * tb, tb), tb), features(k)],
            dst_ref=recv3.at[d - 1, :, features(k)],
            send_sem=s3_send.at[k, d - 1],
            recv_sem=s3_recv.at[k, d - 1],
            device_id=peers[d - 1],
            device_id_type=MESH,
        )

    def second_step(k):
        first_copy(k).wait_recv()
        total = contrib[c, :, features(k)].astype(F32) + recv1[:, features(k)].astype(F32)
        part2[:, features(k)] = total.astype(BF16)
        second_copy(k).start()

    def third_step(k):
        second_copy(k).wait_recv()
        mine = pl.ds(pl.multiple_of(x * half_rows, half_rows), half_rows)
        total = part2[mine, features(k)].astype(F32) + recv2[:, features(k)].astype(F32)
        part3[:, features(k)] = total.astype(BF16)
        for d in range(1, zs):
            third_copy(k, d).start()

    def last_step(k):
        mine = pl.ds(pl.multiple_of(z * tb, tb), tb)
        total = part3[mine, features(k)].astype(F32)
        for d in range(1, zs):
            third_copy(k, d).wait_recv()
            total = total + recv3[d - 1, :, features(k)].astype(F32)
        moe_ref[:, features(k)] = total.astype(BF16)

    def expert():
        lane = lax.broadcasted_iota(jnp.int32, (group, LANES), 1)
        row = lax.broadcasted_iota(jnp.int32, (group, group), 0)
        col = lax.broadcasted_iota(jnp.int32, (group, group), 1)
        before = jnp.where((col < row) & (col // tb == row // tb), 1.0, 0.0).astype(BF16)
        slot_of = lax.broadcasted_iota(jnp.int32, (group, group_slots), 1)
        block = lax.broadcasted_iota(jnp.int32, (group, group_slots), 0) // tb
        wide = min(1024, model)
        for g in range(2):
            extra = tok_all[g, :, model:]
            value = extra.astype(F32)
            gate = (lane == me) | (lane == experts + me)
            gate_col[g] = jnp.sum(jnp.where(gate, value, 0.0), axis=1, keepdims=True)
            pick = lane == 2 * experts + me
            member = jnp.sum(jnp.where(pick, value, 0.0), axis=1, keepdims=True)
            ranks = jnp.dot(before, extra, preferred_element_type=F32)
            rank = jnp.sum(jnp.where(pick, ranks, 0.0), axis=1, keepdims=True)
            target = block.astype(F32) * cap + rank
            chosen = jnp.where((member > 0.5) & (target == slot_of.astype(F32)), 1.0, 0.0)
            chosen_t[g] = chosen.astype(BF16)
            picked = jnp.transpose(chosen).astype(BF16)

            def take(n, carry):
                cols = pl.ds(pl.multiple_of(n * wide, wide), wide)
                rows[g * group_slots : (g + 1) * group_slots, cols] = jnp.dot(
                    picked, tok_all[g, :, cols], preferred_element_type=F32
                ).astype(BF16)
                return carry

            lax.fori_loop(0, model // wide, take, 0)

        def up_step(n, carry):
            slot = lax.rem(n, UP_SLOTS)
            for copy in up_copies(n):
                copy.wait()
            gate = jnp.dot(rows[...], wg_buf[slot], preferred_element_type=F32)
            upward = jnp.dot(rows[...], wu_buf[slot], preferred_element_type=F32)
            value = (gate / (1.0 + jnp.exp(-gate)) * upward).astype(BF16)
            hidden[:, pl.ds(pl.multiple_of(n * ufc, ufc), ufc)] = value

            @pl.when(n + UP_SLOTS < up_steps)
            def _():
                for copy in up_copies(n + UP_SLOTS):
                    copy.start()

            return carry

        lax.fori_loop(0, up_steps, up_step, 0)

        def down_step(n, carry):
            down_copy(n).wait()
            slot = lax.rem(n, DOWN_SLOTS)
            value = jnp.dot(hidden[...], wd_buf[slot], preferred_element_type=F32).astype(BF16)
            for g in range(2):
                spread = jnp.dot(
                    chosen_t[g],
                    value[g * group_slots : (g + 1) * group_slots],
                    preferred_element_type=F32,
                )
                contrib[g, :, features(n)] = (spread * gate_col[g]).astype(BF16)

            @pl.when(n + DOWN_SLOTS < down_steps)
            def _():
                down_copy(n + DOWN_SLOTS).start()

            first_copy(n).start()

            @pl.when(n >= 1)
            def _():
                second_step(n - 1)

            return carry

        lax.fori_loop(0, down_steps, down_step, 0)
        second_step(down_steps - 1)

    def gather_at(i, parity):
        for step, spot in zip(gather_steps, spots):
            if spot % 2 == parity:
                pl.when(i == spot // 2)(step)

    def turn(i, carry):
        gather_at(i, 0)
        pl.when(i == moe_at)(expert)

        @pl.when((i >= moe_at + 3) & (i < moe_at + 3 + down_steps))
        def _():
            last_step(i - moe_at - 3)

        half(i, set_a, set_b)
        gather_at(i, 1)

        @pl.when((i >= moe_at) & (i < moe_at + down_steps))
        def _():
            third_step(i - moe_at)

        half(i, set_b, set_a)
        return carry

    lax.fori_loop(0, turns, turn, 0)

    slot = (turns - 1) % 2
    wv_copy(pairs - 2, wv_a, slot, 0).wait()
    values_of(0, s_b, m_b, l_b, acc_b, True)
    finish(pairs - 2, l_a, acc_a, wv_a, slot)

    def rest(n, carry):
        values_of(n, s_b, m_b, l_b, acc_b, False)
        return carry

    lax.fori_loop(1, z + 1, rest, 0)
    wv_copy(pairs - 1, wv_b, slot, 1).wait()
    finish(pairs - 1, l_b, acc_b, wv_b, slot)

    third_done = min(max(turns - moe_at, 0), down_steps)
    last_done = min(max(turns - moe_at - 3, 0), down_steps)

    def third_rest(k, carry):
        third_step(k)
        return carry

    def last_rest(k, carry):
        last_step(k)
        return carry

    lax.fori_loop(third_done, down_steps, third_rest, 0)
    lax.fori_loop(last_done, down_steps, last_rest, 0)

    for d in range(1, zs):

        @pl.when(z + d < zs)
        def _():
            kv_send_to(z, x, c, partner, d - 1).wait_send()

    for d in range(zs):

        @pl.when(z - d >= 0)
        def _():
            for base in (zs - 1, 2 * zs - 1, 3 * zs - 1):
                kv_send_to(z, x, c, partner, base + d).wait_send()

    for index in range(4 * zs - 1):
        tok_send_to(z, x, c, partner, index).wait_send()

    def drain(k, carry):
        first_copy(k).wait_send()
        second_copy(k).wait_send()
        for d in range(1, zs):
            third_copy(k, d).wait_send()
        return carry

    lax.fori_loop(0, down_steps, drain, 0)


def per_device(queries, latent_kv, w_value, moe_tokens, routes, router, w_gate, w_up, w_down):
    seq_dev, heads, width = queries.shape
    latent, vdim = w_value.shape[1], w_value.shape[2]
    scale = (vdim + width - latent) ** (-0.5)
    tb, top = routes.shape
    ep_size = lax.axis_size("ep")
    experts = router.shape[1]
    assert experts == ep_size and w_gate.shape[0] == 1 and ep_size % 4 == 0
    model, ff = moe_tokens.shape[1], w_gate.shape[2]
    cap = min(tb, 3 * tb * top // (2 * experts))
    zs = ep_size // 4
    wide = -(-width // LANES) * LANES
    keys = ep_size * seq_dev
    group, group_slots = ep_size * tb // 2, ep_size * cap // 2
    ufc = min(256, ff)
    fc = min(512, model)
    down_steps = model // fc
    dims = (zs, heads, width, latent, vdim, seq_dev, tb, model, ff, experts, cap, scale, ufc, fc)
    cols = 2 * seq_dev
    vmem, dma = pltpu.VMEM, pltpu.SemaphoreType.DMA
    scratch = [
        vmem((zs, wide, 4 * seq_dev), BF16),
        vmem((keys, wide), BF16),
        vmem((2, wide, cols), BF16),
        vmem((2, wide, cols), BF16),
        vmem((keys, cols), F32),
        vmem((keys, cols), F32),
        vmem((8, cols), F32),
        vmem((8, cols), F32),
        vmem((8, cols), F32),
        vmem((8, cols), F32),
        vmem((latent, cols), F32),
        vmem((latent, cols), F32),
        vmem((2, 2, latent, vdim), BF16),
        vmem((2, 2, latent, vdim), BF16),
        vmem((2, group, model + LANES), BF16),
        vmem((LANES, LANES), F32),
        vmem((2 * group_slots, model), BF16),
        vmem((2 * group_slots, ff), BF16),
        vmem((2, group, group_slots), BF16),
        vmem((2, group, 1), F32),
        vmem((2, group, model), BF16),
        vmem((group, model), BF16),
        vmem((group, model), BF16),
        vmem((group // 2, model), BF16),
        vmem((group // 2, model), BF16),
        vmem((zs - 1, tb, model), BF16),
        vmem((UP_SLOTS, model, ufc), BF16),
        vmem((UP_SLOTS, model, ufc), BF16),
        vmem((DOWN_SLOTS, ff, fc), BF16),
        dma((2, 2, 2)),
        dma((2, 2)),
        dma((2,)),
        dma((4 * zs - 1,)),
        dma((4 * zs,)),
        dma((4 * zs - 1,)),
        dma((4 * zs,)),
        dma((UP_SLOTS,)),
        dma((UP_SLOTS,)),
        dma((DOWN_SLOTS,)),
        dma((down_steps,)),
        dma((down_steps,)),
        dma((down_steps,)),
        dma((down_steps,)),
        dma((down_steps, zs - 1)),
        dma((down_steps, zs - 1)),
    ]
    hbm = pl.BlockSpec(memory_space=pl.ANY)
    local = pl.BlockSpec(memory_space=pltpu.VMEM)
    attention_out, moe_out = pl.pallas_call(
        functools.partial(layer_kernel, dims),
        in_specs=[hbm, hbm, hbm, hbm, local, local, hbm, hbm, hbm],
        out_specs=[local, local],
        out_shape=[
            jax.ShapeDtypeStruct((seq_dev, heads * vdim), BF16),
            jax.ShapeDtypeStruct((tb, model), BF16),
        ],
        scratch_shapes=scratch,
        compiler_params=pltpu.CompilerParams(
            vmem_limit_bytes=67043328, collective_id=0, has_side_effects=True
        ),
        cost_estimate=pl.CostEstimate(
            flops=heads * seq_dev * keys * (width + latent) * 2,
            bytes_accessed=6 * model * ff,
            transcendentals=heads * seq_dev * keys,
        ),
    )(
        jnp.transpose(queries, (1, 2, 0)),
        jnp.transpose(latent_kv),
        w_value,
        moe_tokens,
        jnp.transpose(routes),
        jnp.transpose(router),
        w_gate,
        w_up,
        w_down,
    )
    if lax.axis_size("node") > 1:
        moe_out = lax.psum_scatter(moe_out, "node", scatter_dimension=1, tiled=True)
    return (attention_out, moe_out)


def solution(mesh):
    placed = (
        P(("groups", "ep"), "node", None),
        P(("groups", "ep"), None),
        P("node", None, None),
        P(("groups", "ep"), None),
        P(("groups", "ep"), None),
        P(),
        P("ep", None, "node"),
        P("ep", None, "node"),
        P("ep", "node", None),
    )
    return jax.shard_map(
        per_device,
        mesh=mesh,
        in_specs=placed,
        out_specs=(P(("groups", "ep"), "node"), P(("groups", "ep"), "node")),
        check_vma=False,
    )
```

```python
import functools

import jax
import jax.numpy as jnp
from jax import lax
from jax.experimental import pallas as pl
from jax.experimental.pallas import tpu as pltpu
from jax.sharding import PartitionSpec as P

ROUTED_SCALE = 2.5
NEGATIVE = -1e30
LOG2E = 1.4426950408889634
MESH = pl.DeviceIdType.MESH
F32 = jnp.float32
BF16 = jnp.bfloat16
LANES = 128
UP_SLOTS = 2
DOWN_SLOTS = 2
MOE_AT = 7


def layer_kernel(dims, q_ref, kv_ref, wv_ref, tok_ref, routes_ref, router_ref, wg_ref, wu_ref,
                 wd_ref, out_ref, moe_ref, *scratch):
    (zs, heads, width, latent, vdim, seq_dev, tb, model, ff, experts, cap, scale, ufc, dfc,
     fc) = dims
    (kvt_all, kv_all, q_a, q_b, s_a, s_b, m_a, m_b, l_a, l_b, acc_a, acc_b, wv_a, wv_b, tok_all,
     aux, rows, hidden, chosen_t, gate_col, contrib, recv1, part2, recv2, part3, recv3, wg_buf,
     wu_buf, wd_buf, q_sem, wv_sem, own_sem, kv_send, kv_recv, tok_send, tok_recv, wg_sem, wu_sem,
     wd_sem, s1_send, s1_recv, s2_send, s2_recv, s3_send, s3_recv) = scratch
    me = lax.axis_index("ep")
    z = me // 4
    x = lax.rem(me // 2, 2)
    c = lax.rem(me, 2)
    chunk = 4 * seq_dev
    pairs = heads // 2
    turns = pairs // 2
    moe_at = min(MOE_AT, turns - 1)
    group = 2 * zs * tb
    group_slots = 2 * zs * cap
    up_steps = ff // ufc
    down_steps = model // dfc
    send_steps = model // fc
    per_down = dfc // fc
    factor = scale * LOG2E

    def at(zz, xx, cc):
        return {"ep": zz * 4 + xx * 2 + cc}

    peers = [at(lax.rem(z + d, zs), x, c) for d in range(1, zs)]
    across = at(z, 1 - x, c)
    partner = at(z, x, 1 - c)

    own_kv = pltpu.make_async_copy(
        kv_ref,
        kvt_all.at[z, pl.ds(0, width), pl.ds(pl.multiple_of((x * 2 + c) * seq_dev, seq_dev), seq_dev)],
        own_sem.at[0],
    )
    own_kv.start()

    def block_row(zz, xx):
        return pl.multiple_of((xx * zs + zz) * tb, tb)

    own_tok = pltpu.make_async_copy(
        tok_ref, tok_all.at[c, pl.ds(block_row(z, x), tb), pl.ds(0, model)], own_sem.at[1]
    )
    own_tok.start()

    def q_copies(pair, buf, slot, base):
        return [
            pltpu.make_async_copy(
                q_ref.at[2 * pair + h],
                buf.at[slot, pl.ds(0, width), pl.ds(h * seq_dev, seq_dev)],
                q_sem.at[base, slot, h],
            )
            for h in range(2)
        ]

    def wv_copy(pair, buf, slot, base):
        return pltpu.make_async_copy(
            wv_ref.at[pl.ds(2 * pair, 2)], buf.at[slot], wv_sem.at[base, slot]
        )

    for copy in q_copies(0, q_a, 0, 0) + q_copies(1, q_b, 0, 1):
        copy.start()

    def up_copies(n):
        slot = lax.rem(n, UP_SLOTS)
        cols = pl.ds(pl.multiple_of(n * ufc, ufc), ufc)
        return (
            pltpu.make_async_copy(wg_ref.at[0, :, cols], wg_buf.at[slot], wg_sem.at[slot]),
            pltpu.make_async_copy(wu_ref.at[0, :, cols], wu_buf.at[slot], wu_sem.at[slot]),
        )

    def down_copy(n):
        slot = lax.rem(n, DOWN_SLOTS)
        cols = pl.ds(pl.multiple_of(n * dfc, dfc), dfc)
        return pltpu.make_async_copy(wd_ref.at[0, :, cols], wd_buf.at[slot], wd_sem.at[slot])

    barrier = pltpu.get_barrier_semaphore()
    for peer in peers + [across, partner]:
        pl.semaphore_signal(barrier, inc=1, device_id=peer, device_id_type=MESH)
    pl.semaphore_wait(barrier, zs + 1)

    def kv_block(zz, xx, cc):
        return kvt_all.at[
            zz, pl.ds(0, width), pl.ds(pl.multiple_of((xx * 2 + cc) * seq_dev, seq_dev), seq_dev)
        ]

    def kv_send_to(zz, xx, cc, target, index):
        block = kv_block(zz, xx, cc)
        return pltpu.make_async_remote_copy(
            src_ref=block,
            dst_ref=block,
            send_sem=kv_send.at[index],
            recv_sem=kv_recv.at[zz * 4 + xx * 2 + cc],
            device_id=target,
            device_id_type=MESH,
        )

    def kv_wait(zz, xx, cc):
        kv_send_to(zz, xx, cc, partner, 0).wait_recv()

    def kv_turn(zz, xx, cc):
        cols = pl.ds(pl.multiple_of((xx * 2 + cc) * seq_dev, seq_dev), seq_dev)
        at_row = pl.ds(pl.multiple_of((zz * 4 + xx * 2 + cc) * seq_dev, seq_dev), seq_dev)
        kv_all[at_row, :] = jnp.transpose(kvt_all[zz, :, cols])

    kvt_all[:, width:, :] = jnp.zeros((zs, kvt_all.shape[1] - width, chunk), BF16)
    for buf in (q_a, q_b):
        buf[:, width:, :] = jnp.zeros((2, buf.shape[1] - width, 2 * seq_dev), BF16)
    own_kv.wait()
    def kv_up(d):
        @pl.when(z + 1 < zs)
        def _():
            kv_send_to(z - d, x, c, at(z + 1, x, c), d).start()

    kv_up(0)
    kv_send_to(z, x, c, across, zs - 1).start()
    kv_send_to(z, x, c, partner, 2 * zs - 1).start()

    own_tok.wait()

    own_rows = pl.ds(block_row(z, x), tb)
    logits = lax.dot_general(
        router_ref[...],
        tok_all[c, own_rows, :model],
        (((1,), (1,)), ((), ())),
        preferred_element_type=F32,
    )
    affinity = jax.nn.sigmoid(logits)
    expert_id = lax.broadcasted_iota(jnp.int32, (experts, tb), 0)
    named = jnp.zeros((experts, tb), F32)
    for k in range(routes_ref.shape[0]):
        named = jnp.where(routes_ref[k : k + 1, :] == expert_id, 1.0, named)
    kept = affinity * named
    gates = ROUTED_SCALE * kept / jnp.sum(kept, axis=0, keepdims=True)
    high = gates.astype(BF16).astype(F32)
    aux[...] = jnp.zeros(aux.shape, F32)
    aux[0:experts, 0:tb] = high
    aux[experts : 2 * experts, 0:tb] = gates - high
    aux[2 * experts : 3 * experts, 0:tb] = named
    tok_all[c, own_rows, model:] = jnp.transpose(aux[...])[:tb].astype(BF16)

    def tok_send_to(zz, xx, cc, target, index):
        block = tok_all.at[cc, pl.ds(block_row(zz, xx), tb)]
        return pltpu.make_async_remote_copy(
            src_ref=block,
            dst_ref=block,
            send_sem=tok_send.at[index],
            recv_sem=tok_recv.at[zz * 4 + xx * 2 + cc],
            device_id=target,
            device_id_type=MESH,
        )

    def tok_wait(zz, xx, cc):
        tok_send_to(zz, xx, cc, partner, 0).wait_recv()

    kv_turn(z, x, c)

    for d in range(1, zs):

        @pl.when(z - d >= 0)
        def _():
            kv_wait(z - d, x, c)
            if d < zs - 1:
                kv_up(d)
            kv_send_to(z - d, x, c, across, zs - 1 + d).start()
            kv_send_to(z - d, x, c, partner, 2 * zs - 1 + d).start()
            kv_turn(z - d, x, c)

    def tok_up(d):
        @pl.when(z + 1 < zs)
        def _():
            tok_send_to(z - d, x, c, at(z + 1, x, c), 3 * zs + d).start()

    def tok_down(d):
        @pl.when(z > 0)
        def _():
            tok_send_to(z + d, x, c, at(z - 1, x, c), 4 * zs - 1 + d).start()

    def tok_aside(zz):
        tok_send_to(zz, x, c, across, zz).start()
        tok_send_to(zz, x, c, partner, zs + zz).start()

    tok_up(0)
    tok_down(0)
    tok_aside(z)

    for n in range(min(UP_SLOTS, up_steps)):
        for copy in up_copies(n):
            copy.start()
    for n in range(min(DOWN_SLOTS, down_steps)):
        down_copy(n).start()

    for d in range(zs):

        @pl.when(z - d >= 0)
        def _():
            kv_wait(z - d, 1 - x, c)
            kv_send_to(z - d, 1 - x, c, partner, 3 * zs - 1 + d).start()
            kv_turn(z - d, 1 - x, c)

    for d in range(zs):
        for xx in (x, 1 - x):

            @pl.when(z - d >= 0)
            def _():
                kv_wait(z - d, xx, 1 - c)
                kv_turn(z - d, xx, 1 - c)

    def scores_of(n, q, s, diagonal):
        base = n * chunk
        score = jnp.dot(kv_all[base : base + chunk, :], q, preferred_element_type=F32)
        if diagonal:
            row = lax.broadcasted_iota(jnp.int32, score.shape, 0)
            col = lax.rem(lax.broadcasted_iota(jnp.int32, score.shape, 1), seq_dev)
            score = jnp.where(row - col <= (x * 2 + c) * seq_dev, score, NEGATIVE)
        s[base : base + chunk, :] = score
        return jnp.max(score.reshape(chunk // 8, 8, score.shape[1]), axis=0)

    def values_of(n, s, high):
        base = n * chunk
        raised = jnp.exp2(s[base : base + chunk, :] * factor - high)
        sums = jnp.sum(raised.reshape(chunk // 8, 8, raised.shape[1]), axis=0)
        value = jnp.dot(kvt_all[n, :latent, :], raised.astype(BF16), preferred_element_type=F32)
        return sums, value

    def sweep(top, q, s, m, s_p, m_p, l_p, acc_p):
        if s_p is not None:
            high = jnp.max(m_p[...], axis=0, keepdims=True) * factor
        tops = sums = value = None
        for n in [top] + list(range(top)):
            if s is not None:
                high8 = scores_of(n, q, s, n == top)
                tops = high8 if tops is None else jnp.maximum(tops, high8)
            if s_p is not None:
                sums_n, value_n = values_of(n, s_p, high)
                sums = sums_n if sums is None else sums + sums_n
                value = value_n if value is None else value + value_n
        if s is not None:
            m[...] = tops
        if s_p is not None:
            l_p[...] = sums
            acc_p[...] = value

    def finish(pair, l, acc, wv, slot):
        totals = jnp.sum(l[...], axis=0, keepdims=True)
        context = (acc[...] * (1.0 / totals)).astype(BF16)
        for h in range(2):
            value = lax.dot_general(
                context[:, h * seq_dev : (h + 1) * seq_dev],
                wv[slot, h],
                (((0,), (0,)), ((), ())),
                preferred_element_type=F32,
            )
            cols = pl.ds(pl.multiple_of((2 * pair + h) * vdim, vdim), vdim)
            out_ref[:, cols] = value.astype(BF16)

    set_a = (q_a, s_a, m_a, l_a, acc_a, wv_a, 0)
    set_b = (q_b, s_b, m_b, l_b, acc_b, wv_b, 1)

    def half(i, cur, prev):
        q, s, m, l, acc, wv, parity = cur
        _, s_p, m_p, l_p, acc_p, _, _ = prev
        pair = 2 * i + parity
        slot = lax.rem(i, 2)
        other = 1 - slot
        for copy in q_copies(pair, q, slot, parity):
            copy.wait()

        @pl.when(i + 1 < turns)
        def _():
            for copy in q_copies(pair + 2, q, other, parity):
                copy.start()

        @pl.when(i >= 1)
        def _():
            wv_copy(pair - 2, wv, other, parity).wait()

        wv_copy(pair, wv, slot, parity).start()
        for top in range(zs):

            @pl.when(z == top)
            def _():
                sweep(top, q[slot], s, m, s_p, m_p, l_p, acc_p)
                finish(jnp.maximum(pair - 2, 0), l, acc, wv, other)

    def from_levels(d):
        @pl.when(z - d >= 0)
        def _():
            tok_wait(z - d, x, c)
            if d < zs - 1:
                tok_up(d)
            tok_aside(z - d)

        @pl.when(z + d < zs)
        def _():
            tok_wait(z + d, x, c)
            if d < zs - 1:
                tok_down(d)
            tok_aside(z + d)

    def pass_on(zz):
        tok_wait(zz, 1 - x, c)
        tok_send_to(zz, 1 - x, c, partner, 2 * zs + zz).start()

    def from_across(d):
        if d == 0:
            pass_on(z)
        else:
            pl.when(z - d >= 0)(lambda: pass_on(z - d))
            pl.when(z + d < zs)(lambda: pass_on(z + d))

    def from_partner():
        for d in range(zs):
            for xx in (x, 1 - x):
                tok_wait(lax.rem(z + d, zs), xx, 1 - c)

    gather_steps = []
    for d in range(1, zs):
        gather_steps += [functools.partial(from_levels, d), functools.partial(from_across, d - 1)]
    gather_steps += [functools.partial(from_across, zs - 1), from_partner]
    spots = [
        (2 * moe_at * a) // (len(gather_steps) - 1) for a in range(len(gather_steps))
    ]

    def features(k):
        return pl.ds(pl.multiple_of(k * fc, fc), fc)

    half_rows = group // 2

    def first_copy(k):
        return pltpu.make_async_remote_copy(
            src_ref=contrib.at[1 - c, :, features(k)],
            dst_ref=recv1.at[:, features(k)],
            send_sem=s1_send.at[k],
            recv_sem=s1_recv.at[k],
            device_id=partner,
            device_id_type=MESH,
        )

    def second_copy(k):
        away = pl.ds(pl.multiple_of((1 - x) * half_rows, half_rows), half_rows)
        return pltpu.make_async_remote_copy(
            src_ref=part2.at[away, features(k)],
            dst_ref=recv2.at[:, features(k)],
            send_sem=s2_send.at[k],
            recv_sem=s2_recv.at[k],
            device_id=across,
            device_id_type=MESH,
        )

    def third_copy(k, d):
        to = lax.rem(z + d, zs)
        return pltpu.make_async_remote_copy(
            src_ref=part3.at[pl.ds(pl.multiple_of(to * tb, tb), tb), features(k)],
            dst_ref=recv3.at[d - 1, :, features(k)],
            send_sem=s3_send.at[k, d - 1],
            recv_sem=s3_recv.at[k, d - 1],
            device_id=peers[d - 1],
            device_id_type=MESH,
        )

    def second_step(k):
        first_copy(k).wait_recv()
        total = contrib[c, :, features(k)].astype(F32) + recv1[:, features(k)].astype(F32)
        part2[:, features(k)] = total.astype(BF16)
        second_copy(k).start()

    def third_step(k):
        second_copy(k).wait_recv()
        mine = pl.ds(pl.multiple_of(x * half_rows, half_rows), half_rows)
        total = part2[mine, features(k)].astype(F32) + recv2[:, features(k)].astype(F32)
        part3[:, features(k)] = total.astype(BF16)
        for d in range(1, zs):
            third_copy(k, d).start()

    def last_step(k):
        mine = pl.ds(pl.multiple_of(z * tb, tb), tb)
        total = part3[mine, features(k)].astype(F32)
        for d in range(1, zs):
            third_copy(k, d).wait_recv()
            total = total + recv3[d - 1, :, features(k)].astype(F32)
        moe_ref[:, features(k)] = total.astype(BF16)

    def expert():
        lane = lax.broadcasted_iota(jnp.int32, (group, LANES), 1)
        row = lax.broadcasted_iota(jnp.int32, (group, group), 0)
        col = lax.broadcasted_iota(jnp.int32, (group, group), 1)
        before = jnp.where((col < row) & (col // tb == row // tb), 1.0, 0.0).astype(BF16)
        slot_of = lax.broadcasted_iota(jnp.int32, (group, group_slots), 1)
        block = lax.broadcasted_iota(jnp.int32, (group, group_slots), 0) // tb
        wide = min(1024, model)
        for g in range(2):
            extra = tok_all[g, :, model:]
            value = extra.astype(F32)
            gate = (lane == me) | (lane == experts + me)
            gate_col[g] = jnp.sum(jnp.where(gate, value, 0.0), axis=1, keepdims=True)
            pick = lane == 2 * experts + me
            member = jnp.sum(jnp.where(pick, value, 0.0), axis=1, keepdims=True)
            ranks = jnp.dot(before, extra, preferred_element_type=F32)
            rank = jnp.sum(jnp.where(pick, ranks, 0.0), axis=1, keepdims=True)
            target = block.astype(F32) * cap + rank
            chosen = jnp.where((member > 0.5) & (target == slot_of.astype(F32)), 1.0, 0.0)
            chosen_t[g] = chosen.astype(BF16)
            picked = jnp.transpose(chosen).astype(BF16)

            def take(n, carry):
                cols = pl.ds(pl.multiple_of(n * wide, wide), wide)
                rows[g * group_slots : (g + 1) * group_slots, cols] = jnp.dot(
                    picked, tok_all[g, :, cols], preferred_element_type=F32
                ).astype(BF16)
                return carry

            lax.fori_loop(0, model // wide, take, 0)

        def up_step(n, carry):
            slot = lax.rem(n, UP_SLOTS)
            for copy in up_copies(n):
                copy.wait()
            gate = jnp.dot(rows[...], wg_buf[slot], preferred_element_type=F32)
            upward = jnp.dot(rows[...], wu_buf[slot], preferred_element_type=F32)
            value = (gate / (1.0 + jnp.exp(-gate)) * upward).astype(BF16)
            hidden[:, pl.ds(pl.multiple_of(n * ufc, ufc), ufc)] = value

            @pl.when(n + UP_SLOTS < up_steps)
            def _():
                for copy in up_copies(n + UP_SLOTS):
                    copy.start()

            return carry

        lax.fori_loop(0, up_steps, up_step, 0)

        def down_step(n, carry):
            down_copy(n).wait()
            slot = lax.rem(n, DOWN_SLOTS)
            value = jnp.dot(hidden[...], wd_buf[slot], preferred_element_type=F32).astype(BF16)
            for g in range(2):
                spread = jnp.dot(
                    chosen_t[g],
                    value[g * group_slots : (g + 1) * group_slots],
                    preferred_element_type=F32,
                )
                whole = pl.ds(pl.multiple_of(n * dfc, dfc), dfc)
                contrib[g, :, whole] = (spread * gate_col[g]).astype(BF16)

            @pl.when(n + DOWN_SLOTS < down_steps)
            def _():
                down_copy(n + DOWN_SLOTS).start()

            for k in range(per_down):
                first_copy(n * per_down + k).start()

            @pl.when(n >= 1)
            def _():
                for k in range(per_down):
                    second_step((n - 1) * per_down + k)

            return carry

        lax.fori_loop(0, down_steps, down_step, 0)
        for k in range(send_steps - per_down, send_steps):
            second_step(k)

    def gather_at(i, parity):
        for step, spot in zip(gather_steps, spots):
            if spot % 2 == parity:
                pl.when(i == spot // 2)(step)

    def turn(i, carry):
        gather_at(i, 0)
        pl.when(i == moe_at)(expert)

        @pl.when((i >= moe_at + 3) & (i < moe_at + 3 + send_steps))
        def _():
            last_step(i - moe_at - 3)

        half(i, set_a, set_b)
        gather_at(i, 1)

        @pl.when((i >= moe_at) & (i < moe_at + send_steps))
        def _():
            third_step(i - moe_at)

        half(i, set_b, set_a)
        return carry

    lax.fori_loop(0, turns, turn, 0)

    slot = (turns - 1) % 2
    wv_copy(pairs - 2, wv_a, slot, 0).wait()
    finish(pairs - 2, l_a, acc_a, wv_a, slot)
    for top in range(zs):
        pl.when(z == top)(
            functools.partial(sweep, top, None, None, None, s_b, m_b, l_b, acc_b)
        )

    wv_copy(pairs - 1, wv_b, slot, 1).wait()
    finish(pairs - 1, l_b, acc_b, wv_b, slot)

    third_done = min(max(turns - moe_at, 0), send_steps)
    last_done = min(max(turns - moe_at - 3, 0), send_steps)

    def third_rest(k, carry):
        third_step(k)
        return carry

    def last_rest(k, carry):
        last_step(k)
        return carry

    lax.fori_loop(third_done, send_steps, third_rest, 0)
    lax.fori_loop(last_done, send_steps, last_rest, 0)

    for d in range(zs - 1):

        @pl.when((z + 1 < zs) & (z - d >= 0))
        def _():
            kv_send_to(z, x, c, partner, d).wait_send()

        @pl.when((z + 1 < zs) & (z - d >= 0))
        def _():
            tok_send_to(z, x, c, partner, 3 * zs + d).wait_send()

        @pl.when((z > 0) & (z + d < zs))
        def _():
            tok_send_to(z, x, c, partner, 4 * zs - 1 + d).wait_send()

    for d in range(zs):

        @pl.when(z - d >= 0)
        def _():
            for base in (zs - 1, 2 * zs - 1, 3 * zs - 1):
                kv_send_to(z, x, c, partner, base + d).wait_send()

    for index in range(3 * zs):
        tok_send_to(z, x, c, partner, index).wait_send()

    def drain(k, carry):
        first_copy(k).wait_send()
        second_copy(k).wait_send()
        for d in range(1, zs):
            third_copy(k, d).wait_send()
        return carry

    lax.fori_loop(0, send_steps, drain, 0)


def per_device(queries, latent_kv, w_value, moe_tokens, routes, router, w_gate, w_up, w_down):
    seq_dev, heads, width = queries.shape
    latent, vdim = w_value.shape[1], w_value.shape[2]
    scale = (vdim + width - latent) ** (-0.5)
    tb, top = routes.shape
    ep_size = lax.axis_size("ep")
    experts = router.shape[1]
    assert experts == ep_size and w_gate.shape[0] == 1 and ep_size % 4 == 0
    model, ff = moe_tokens.shape[1], w_gate.shape[2]
    cap = min(tb, 3 * tb * top // (2 * experts))
    zs = ep_size // 4
    wide = -(-width // LANES) * LANES
    keys = ep_size * seq_dev
    group, group_slots = ep_size * tb // 2, ep_size * cap // 2
    ufc = min(512, ff)
    dfc = min(1024, model)
    fc = min(512, model)
    send_steps = model // fc
    dims = (zs, heads, width, latent, vdim, seq_dev, tb, model, ff, experts, cap, scale, ufc, dfc,
            fc)
    cols = 2 * seq_dev
    vmem, dma = pltpu.VMEM, pltpu.SemaphoreType.DMA
    scratch = [
        vmem((zs, wide, 4 * seq_dev), BF16),
        vmem((keys, wide), BF16),
        vmem((2, wide, cols), BF16),
        vmem((2, wide, cols), BF16),
        vmem((keys, cols), F32),
        vmem((keys, cols), F32),
        vmem((8, cols), F32),
        vmem((8, cols), F32),
        vmem((8, cols), F32),
        vmem((8, cols), F32),
        vmem((latent, cols), F32),
        vmem((latent, cols), F32),
        vmem((2, 2, latent, vdim), BF16),
        vmem((2, 2, latent, vdim), BF16),
        vmem((2, group, model + LANES), BF16),
        vmem((LANES, LANES), F32),
        vmem((2 * group_slots, model), BF16),
        vmem((2 * group_slots, ff), BF16),
        vmem((2, group, group_slots), BF16),
        vmem((2, group, 1), F32),
        vmem((2, group, model), BF16),
        vmem((group, model), BF16),
        vmem((group, model), BF16),
        vmem((group // 2, model), BF16),
        vmem((group // 2, model), BF16),
        vmem((zs - 1, tb, model), BF16),
        vmem((UP_SLOTS, model, ufc), BF16),
        vmem((UP_SLOTS, model, ufc), BF16),
        vmem((DOWN_SLOTS, ff, dfc), BF16),
        dma((2, 2, 2)),
        dma((2, 2)),
        dma((2,)),
        dma((4 * zs - 1,)),
        dma((4 * zs,)),
        dma((5 * zs - 2,)),
        dma((4 * zs,)),
        dma((UP_SLOTS,)),
        dma((UP_SLOTS,)),
        dma((DOWN_SLOTS,)),
        dma((send_steps,)),
        dma((send_steps,)),
        dma((send_steps,)),
        dma((send_steps,)),
        dma((send_steps, zs - 1)),
        dma((send_steps, zs - 1)),
    ]
    hbm = pl.BlockSpec(memory_space=pl.ANY)
    local = pl.BlockSpec(memory_space=pltpu.VMEM)
    attention_out, moe_out = pl.pallas_call(
        functools.partial(layer_kernel, dims),
        in_specs=[hbm, hbm, hbm, hbm, local, local, hbm, hbm, hbm],
        out_specs=[local, local],
        out_shape=[
            jax.ShapeDtypeStruct((seq_dev, heads * vdim), BF16),
            jax.ShapeDtypeStruct((tb, model), BF16),
        ],
        scratch_shapes=scratch,
        compiler_params=pltpu.CompilerParams(
            vmem_limit_bytes=67043328, collective_id=0, has_side_effects=True
        ),
        cost_estimate=pl.CostEstimate(
            flops=heads * seq_dev * keys * (width + latent) * 2,
            bytes_accessed=6 * model * ff,
            transcendentals=heads * seq_dev * keys,
        ),
    )(
        jnp.transpose(queries, (1, 2, 0)),
        jnp.transpose(latent_kv),
        w_value,
        moe_tokens,
        jnp.transpose(routes),
        jnp.transpose(router),
        w_gate,
        w_up,
        w_down,
    )
    if lax.axis_size("node") > 1:
        moe_out = lax.psum_scatter(moe_out, "node", scatter_dimension=1, tiled=True)
    return (attention_out, moe_out)


def solution(mesh):
    placed = (
        P(("groups", "ep"), "node", None),
        P(("groups", "ep"), None),
        P("node", None, None),
        P(("groups", "ep"), None),
        P(("groups", "ep"), None),
        P(),
        P("ep", None, "node"),
        P("ep", None, "node"),
        P("ep", "node", None),
    )
    return jax.shard_map(
        per_device,
        mesh=mesh,
        in_specs=placed,
        out_specs=(P(("groups", "ep"), "node"), P(("groups", "ep"), "node")),
        check_vma=False,
    )
```

```python
import functools

import jax
import jax.numpy as jnp
from jax import lax
from jax.experimental import pallas as pl
from jax.experimental.pallas import tpu as pltpu
from jax.sharding import PartitionSpec as P

ROUTED_SCALE = 2.5
NEGATIVE = -1e30
LOG2E = 1.4426950408889634
MESH = pl.DeviceIdType.MESH
F32 = jnp.float32
BF16 = jnp.bfloat16
LANES = 128
UP_SLOTS = 2
DOWN_SLOTS = 2
MOE_AT = 7
KV_PIECES = 2


def layer_kernel(dims, q_ref, kv_ref, wv_ref, tok_ref, routes_ref, router_ref, wg_ref, wu_ref,
                 wd_ref, out_ref, moe_ref, *scratch):
    (zs, heads, width, latent, vdim, seq_dev, tb, model, ff, experts, cap, scale, ufc, dfc,
     fc) = dims
    (kvt_all, kv_all, q_a, q_b, s_a, s_b, m_a, m_b, l_a, l_b, acc_a, acc_b, wv_a, wv_b, tok_all,
     aux, rows, hidden, chosen_t, gate_col, contrib, recv1, part2, recv2, part3, recv3, wg_buf,
     wu_buf, wd_buf, q_sem, wv_sem, own_sem, kv_send, kv_recv, tok_send, tok_recv, wg_sem, wu_sem,
     wd_sem, s1_send, s1_recv, s2_send, s2_recv, s3_send, s3_recv) = scratch
    me = lax.axis_index("ep")
    z = me // 4
    x = lax.rem(me // 2, 2)
    c = lax.rem(me, 2)
    chunk = 4 * seq_dev
    pairs = heads // 2
    turns = pairs // 2
    moe_at = min(MOE_AT, turns - 1)
    group = 2 * zs * tb
    group_slots = 2 * zs * cap
    up_steps = ff // ufc
    down_steps = model // dfc
    send_steps = model // fc
    per_down = dfc // fc
    factor = scale * LOG2E

    def at(zz, xx, cc):
        return {"ep": zz * 4 + xx * 2 + cc}

    peers = [at(lax.rem(z + d, zs), x, c) for d in range(1, zs)]
    across = at(z, 1 - x, c)
    partner = at(z, x, 1 - c)

    own_kv = pltpu.make_async_copy(
        kv_ref,
        kvt_all.at[z, pl.ds(0, width), pl.ds(pl.multiple_of((x * 2 + c) * seq_dev, seq_dev), seq_dev)],
        own_sem.at[0],
    )
    own_kv.start()

    def block_row(zz, xx):
        return pl.multiple_of((xx * zs + zz) * tb, tb)

    own_tok = pltpu.make_async_copy(
        tok_ref, tok_all.at[c, pl.ds(block_row(z, x), tb), pl.ds(0, model)], own_sem.at[1]
    )
    own_tok.start()

    def q_copies(pair, buf, slot, base):
        return [
            pltpu.make_async_copy(
                q_ref.at[2 * pair + h],
                buf.at[slot, pl.ds(0, width), pl.ds(h * seq_dev, seq_dev)],
                q_sem.at[base, slot, h],
            )
            for h in range(2)
        ]

    def wv_copy(pair, buf, slot, base):
        return pltpu.make_async_copy(
            wv_ref.at[pl.ds(2 * pair, 2)], buf.at[slot], wv_sem.at[base, slot]
        )

    for copy in q_copies(0, q_a, 0, 0) + q_copies(1, q_b, 0, 1):
        copy.start()

    def up_copies(n):
        slot = lax.rem(n, UP_SLOTS)
        cols = pl.ds(pl.multiple_of(n * ufc, ufc), ufc)
        return (
            pltpu.make_async_copy(wg_ref.at[0, :, cols], wg_buf.at[slot], wg_sem.at[slot]),
            pltpu.make_async_copy(wu_ref.at[0, :, cols], wu_buf.at[slot], wu_sem.at[slot]),
        )

    def down_copy(n):
        slot = lax.rem(n, DOWN_SLOTS)
        cols = pl.ds(pl.multiple_of(n * dfc, dfc), dfc)
        return pltpu.make_async_copy(wd_ref.at[0, :, cols], wd_buf.at[slot], wd_sem.at[slot])

    barrier = pltpu.get_barrier_semaphore()
    for peer in peers + [across, partner]:
        pl.semaphore_signal(barrier, inc=1, device_id=peer, device_id_type=MESH)
    pl.semaphore_wait(barrier, zs + 1)

    piece = width // KV_PIECES

    def kv_send_to(zz, xx, cc, target, index, p):
        block = kvt_all.at[
            zz,
            pl.ds(p * piece, piece),
            pl.ds(pl.multiple_of((xx * 2 + cc) * seq_dev, seq_dev), seq_dev),
        ]
        return pltpu.make_async_remote_copy(
            src_ref=block,
            dst_ref=block,
            send_sem=kv_send.at[index, p],
            recv_sem=kv_recv.at[zz * 4 + xx * 2 + cc, p],
            device_id=target,
            device_id_type=MESH,
        )

    def kv_wait(zz, xx, cc, p):
        kv_send_to(zz, xx, cc, partner, 0, p).wait_recv()

    def kv_turn(zz, xx, cc):
        cols = pl.ds(pl.multiple_of((xx * 2 + cc) * seq_dev, seq_dev), seq_dev)
        at_row = pl.ds(pl.multiple_of((zz * 4 + xx * 2 + cc) * seq_dev, seq_dev), seq_dev)
        kv_all[at_row, :] = jnp.transpose(kvt_all[zz, :, cols])

    kvt_all[:, width:, :] = jnp.zeros((zs, kvt_all.shape[1] - width, chunk), BF16)
    for buf in (q_a, q_b):
        buf[:, width:, :] = jnp.zeros((2, buf.shape[1] - width, 2 * seq_dev), BF16)
    own_kv.wait()
    def kv_up(d, p):
        @pl.when(z + 1 < zs)
        def _():
            kv_send_to(z - d, x, c, at(z + 1, x, c), d, p).start()

    for p in range(KV_PIECES):
        kv_up(0, p)
        kv_send_to(z, x, c, across, zs - 1, p).start()
        kv_send_to(z, x, c, partner, 2 * zs - 1, p).start()

    own_tok.wait()

    own_rows = pl.ds(block_row(z, x), tb)
    logits = lax.dot_general(
        router_ref[...],
        tok_all[c, own_rows, :model],
        (((1,), (1,)), ((), ())),
        preferred_element_type=F32,
    )
    affinity = jax.nn.sigmoid(logits)
    expert_id = lax.broadcasted_iota(jnp.int32, (experts, tb), 0)
    named = jnp.zeros((experts, tb), F32)
    for k in range(routes_ref.shape[0]):
        named = jnp.where(routes_ref[k : k + 1, :] == expert_id, 1.0, named)
    kept = affinity * named
    gates = ROUTED_SCALE * kept / jnp.sum(kept, axis=0, keepdims=True)
    high = gates.astype(BF16).astype(F32)
    aux[...] = jnp.zeros(aux.shape, F32)
    aux[0:experts, 0:tb] = high
    aux[experts : 2 * experts, 0:tb] = gates - high
    aux[2 * experts : 3 * experts, 0:tb] = named
    tok_all[c, own_rows, model:] = jnp.transpose(aux[...])[:tb].astype(BF16)

    def tok_send_to(zz, xx, cc, target, index):
        block = tok_all.at[cc, pl.ds(block_row(zz, xx), tb)]
        return pltpu.make_async_remote_copy(
            src_ref=block,
            dst_ref=block,
            send_sem=tok_send.at[index],
            recv_sem=tok_recv.at[zz * 4 + xx * 2 + cc],
            device_id=target,
            device_id_type=MESH,
        )

    def tok_wait(zz, xx, cc):
        tok_send_to(zz, xx, cc, partner, 0).wait_recv()

    kv_turn(z, x, c)

    for d in range(1, zs):

        @pl.when(z - d >= 0)
        def _():
            for p in range(KV_PIECES):
                kv_wait(z - d, x, c, p)
                if d < zs - 1:
                    kv_up(d, p)
                kv_send_to(z - d, x, c, across, zs - 1 + d, p).start()
                kv_send_to(z - d, x, c, partner, 2 * zs - 1 + d, p).start()
            kv_turn(z - d, x, c)

    def tok_up(d):
        @pl.when(z + 1 < zs)
        def _():
            tok_send_to(z - d, x, c, at(z + 1, x, c), 3 * zs + d).start()

    def tok_down(d):
        @pl.when(z > 0)
        def _():
            tok_send_to(z + d, x, c, at(z - 1, x, c), 4 * zs - 1 + d).start()

    def tok_aside(zz):
        tok_send_to(zz, x, c, across, zz).start()
        tok_send_to(zz, x, c, partner, zs + zz).start()

    tok_up(0)
    tok_down(0)
    tok_aside(z)

    for n in range(min(UP_SLOTS, up_steps)):
        for copy in up_copies(n):
            copy.start()
    for n in range(min(DOWN_SLOTS, down_steps)):
        down_copy(n).start()

    for d in range(zs):

        @pl.when(z - d >= 0)
        def _():
            for p in range(KV_PIECES):
                kv_wait(z - d, 1 - x, c, p)
                kv_send_to(z - d, 1 - x, c, partner, 3 * zs - 1 + d, p).start()
            kv_turn(z - d, 1 - x, c)

    for d in range(zs):
        for xx in (x, 1 - x):

            @pl.when(z - d >= 0)
            def _():
                for p in range(KV_PIECES):
                    kv_wait(z - d, xx, 1 - c, p)
                kv_turn(z - d, xx, 1 - c)

    def scores_of(n, q, s, diagonal):
        base = n * chunk
        score = jnp.dot(kv_all[base : base + chunk, :], q, preferred_element_type=F32)
        if diagonal:
            row = lax.broadcasted_iota(jnp.int32, score.shape, 0)
            col = lax.rem(lax.broadcasted_iota(jnp.int32, score.shape, 1), seq_dev)
            score = jnp.where(row - col <= (x * 2 + c) * seq_dev, score, NEGATIVE)
        s[base : base + chunk, :] = score
        return jnp.max(score.reshape(chunk // 8, 8, score.shape[1]), axis=0)

    def values_of(n, s, high):
        base = n * chunk
        raised = jnp.exp2(s[base : base + chunk, :] * factor - high)
        sums = jnp.sum(raised.reshape(chunk // 8, 8, raised.shape[1]), axis=0)
        value = jnp.dot(kvt_all[n, :latent, :], raised.astype(BF16), preferred_element_type=F32)
        return sums, value

    def sweep(top, q, s, m, s_p, m_p, l_p, acc_p):
        if s_p is not None:
            high = jnp.max(m_p[...], axis=0, keepdims=True) * factor
        tops = sums = value = None
        for n in [top] + list(range(top)):
            if s is not None:
                high8 = scores_of(n, q, s, n == top)
                tops = high8 if tops is None else jnp.maximum(tops, high8)
            if s_p is not None:
                sums_n, value_n = values_of(n, s_p, high)
                sums = sums_n if sums is None else sums + sums_n
                value = value_n if value is None else value + value_n
        if s is not None:
            m[...] = tops
        if s_p is not None:
            l_p[...] = sums
            acc_p[...] = value

    def finish(pair, l, acc, wv, slot):
        totals = jnp.sum(l[...], axis=0, keepdims=True)
        context = (acc[...] * (1.0 / totals)).astype(BF16)
        for h in range(2):
            value = lax.dot_general(
                context[:, h * seq_dev : (h + 1) * seq_dev],
                wv[slot, h],
                (((0,), (0,)), ((), ())),
                preferred_element_type=F32,
            )
            cols = pl.ds(pl.multiple_of((2 * pair + h) * vdim, vdim), vdim)
            out_ref[:, cols] = value.astype(BF16)

    set_a = (q_a, s_a, m_a, l_a, acc_a, wv_a, 0)
    set_b = (q_b, s_b, m_b, l_b, acc_b, wv_b, 1)

    def half(i, cur, prev):
        q, s, m, l, acc, wv, parity = cur
        _, s_p, m_p, l_p, acc_p, _, _ = prev
        pair = 2 * i + parity
        slot = lax.rem(i, 2)
        other = 1 - slot
        for copy in q_copies(pair, q, slot, parity):
            copy.wait()

        @pl.when(i + 1 < turns)
        def _():
            for copy in q_copies(pair + 2, q, other, parity):
                copy.start()

        @pl.when(i >= 1)
        def _():
            wv_copy(pair - 2, wv, other, parity).wait()

        wv_copy(pair, wv, slot, parity).start()
        for top in range(zs):

            @pl.when(z == top)
            def _():
                sweep(top, q[slot], s, m, s_p, m_p, l_p, acc_p)
                finish(jnp.maximum(pair - 2, 0), l, acc, wv, other)

    def from_levels(d):
        @pl.when(z - d >= 0)
        def _():
            tok_wait(z - d, x, c)
            if d < zs - 1:
                tok_up(d)
            tok_aside(z - d)

        @pl.when(z + d < zs)
        def _():
            tok_wait(z + d, x, c)
            if d < zs - 1:
                tok_down(d)
            tok_aside(z + d)

    def pass_on(zz):
        tok_wait(zz, 1 - x, c)
        tok_send_to(zz, 1 - x, c, partner, 2 * zs + zz).start()

    def from_across(d):
        if d == 0:
            pass_on(z)
        else:
            pl.when(z - d >= 0)(lambda: pass_on(z - d))
            pl.when(z + d < zs)(lambda: pass_on(z + d))

    def from_partner():
        for d in range(zs):
            for xx in (x, 1 - x):
                tok_wait(lax.rem(z + d, zs), xx, 1 - c)

    gather_steps = []
    for d in range(1, zs):
        gather_steps += [functools.partial(from_levels, d), functools.partial(from_across, d - 1)]
    gather_steps += [functools.partial(from_across, zs - 1), from_partner]
    spots = [
        (2 * moe_at * a) // (len(gather_steps) - 1) for a in range(len(gather_steps))
    ]

    def features(k):
        return pl.ds(pl.multiple_of(k * fc, fc), fc)

    half_rows = group // 2

    def first_copy(k):
        return pltpu.make_async_remote_copy(
            src_ref=contrib.at[1 - c, :, features(k)],
            dst_ref=recv1.at[:, features(k)],
            send_sem=s1_send.at[k],
            recv_sem=s1_recv.at[k],
            device_id=partner,
            device_id_type=MESH,
        )

    def second_copy(k):
        away = pl.ds(pl.multiple_of((1 - x) * half_rows, half_rows), half_rows)
        return pltpu.make_async_remote_copy(
            src_ref=part2.at[away, features(k)],
            dst_ref=recv2.at[:, features(k)],
            send_sem=s2_send.at[k],
            recv_sem=s2_recv.at[k],
            device_id=across,
            device_id_type=MESH,
        )

    def third_copy(k, d):
        to = lax.rem(z + d, zs)
        return pltpu.make_async_remote_copy(
            src_ref=part3.at[pl.ds(pl.multiple_of(to * tb, tb), tb), features(k)],
            dst_ref=recv3.at[d - 1, :, features(k)],
            send_sem=s3_send.at[k, d - 1],
            recv_sem=s3_recv.at[k, d - 1],
            device_id=peers[d - 1],
            device_id_type=MESH,
        )

    def second_step(k):
        first_copy(k).wait_recv()
        total = contrib[c, :, features(k)].astype(F32) + recv1[:, features(k)].astype(F32)
        part2[:, features(k)] = total.astype(BF16)
        second_copy(k).start()

    def third_step(k):
        second_copy(k).wait_recv()
        mine = pl.ds(pl.multiple_of(x * half_rows, half_rows), half_rows)
        total = part2[mine, features(k)].astype(F32) + recv2[:, features(k)].astype(F32)
        part3[:, features(k)] = total.astype(BF16)
        for d in range(1, zs):
            third_copy(k, d).start()

    def last_step(k):
        mine = pl.ds(pl.multiple_of(z * tb, tb), tb)
        total = part3[mine, features(k)].astype(F32)
        for d in range(1, zs):
            third_copy(k, d).wait_recv()
            total = total + recv3[d - 1, :, features(k)].astype(F32)
        moe_ref[:, features(k)] = total.astype(BF16)

    def expert():
        lane = lax.broadcasted_iota(jnp.int32, (group, LANES), 1)
        row = lax.broadcasted_iota(jnp.int32, (group, group), 0)
        col = lax.broadcasted_iota(jnp.int32, (group, group), 1)
        before = jnp.where((col < row) & (col // tb == row // tb), 1.0, 0.0).astype(BF16)
        slot_of = lax.broadcasted_iota(jnp.int32, (group, group_slots), 1)
        block = lax.broadcasted_iota(jnp.int32, (group, group_slots), 0) // tb
        wide = min(1024, model)
        for g in range(2):
            extra = tok_all[g, :, model:]
            value = extra.astype(F32)
            gate = (lane == me) | (lane == experts + me)
            gate_col[g] = jnp.sum(jnp.where(gate, value, 0.0), axis=1, keepdims=True)
            pick = lane == 2 * experts + me
            member = jnp.sum(jnp.where(pick, value, 0.0), axis=1, keepdims=True)
            ranks = jnp.dot(before, extra, preferred_element_type=F32)
            rank = jnp.sum(jnp.where(pick, ranks, 0.0), axis=1, keepdims=True)
            target = block.astype(F32) * cap + rank
            chosen = jnp.where((member > 0.5) & (target == slot_of.astype(F32)), 1.0, 0.0)
            chosen_t[g] = chosen.astype(BF16)
            picked = jnp.transpose(chosen).astype(BF16)

            def take(n, carry):
                cols = pl.ds(pl.multiple_of(n * wide, wide), wide)
                rows[g * group_slots : (g + 1) * group_slots, cols] = jnp.dot(
                    picked, tok_all[g, :, cols], preferred_element_type=F32
                ).astype(BF16)
                return carry

            lax.fori_loop(0, model // wide, take, 0)

        def up_step(n, carry):
            slot = lax.rem(n, UP_SLOTS)
            for copy in up_copies(n):
                copy.wait()
            gate = jnp.dot(rows[...], wg_buf[slot], preferred_element_type=F32)
            upward = jnp.dot(rows[...], wu_buf[slot], preferred_element_type=F32)
            value = (gate / (1.0 + jnp.exp(-gate)) * upward).astype(BF16)
            hidden[:, pl.ds(pl.multiple_of(n * ufc, ufc), ufc)] = value

            @pl.when(n + UP_SLOTS < up_steps)
            def _():
                for copy in up_copies(n + UP_SLOTS):
                    copy.start()

            return carry

        lax.fori_loop(0, up_steps, up_step, 0)

        def down_step(n, carry):
            down_copy(n).wait()
            slot = lax.rem(n, DOWN_SLOTS)
            value = jnp.dot(hidden[...], wd_buf[slot], preferred_element_type=F32).astype(BF16)
            for g in range(2):
                spread = jnp.dot(
                    chosen_t[g],
                    value[g * group_slots : (g + 1) * group_slots],
                    preferred_element_type=F32,
                )
                whole = pl.ds(pl.multiple_of(n * dfc, dfc), dfc)
                contrib[g, :, whole] = (spread * gate_col[g]).astype(BF16)

            @pl.when(n + DOWN_SLOTS < down_steps)
            def _():
                down_copy(n + DOWN_SLOTS).start()

            for k in range(per_down):
                first_copy(n * per_down + k).start()

            @pl.when(n >= 1)
            def _():
                for k in range(per_down):
                    second_step((n - 1) * per_down + k)

            return carry

        lax.fori_loop(0, down_steps, down_step, 0)
        for k in range(send_steps - per_down, send_steps):
            second_step(k)

    def gather_at(i, parity):
        for step, spot in zip(gather_steps, spots):
            if spot % 2 == parity:
                pl.when(i == spot // 2)(step)

    def turn(i, carry):
        gather_at(i, 0)
        pl.when(i == moe_at)(expert)

        @pl.when((i >= moe_at + 3) & (i < moe_at + 3 + send_steps))
        def _():
            last_step(i - moe_at - 3)

        half(i, set_a, set_b)
        gather_at(i, 1)

        @pl.when((i >= moe_at) & (i < moe_at + send_steps))
        def _():
            third_step(i - moe_at)

        half(i, set_b, set_a)
        return carry

    lax.fori_loop(0, turns, turn, 0)

    slot = (turns - 1) % 2
    wv_copy(pairs - 2, wv_a, slot, 0).wait()
    finish(pairs - 2, l_a, acc_a, wv_a, slot)
    for top in range(zs):
        pl.when(z == top)(
            functools.partial(sweep, top, None, None, None, s_b, m_b, l_b, acc_b)
        )

    wv_copy(pairs - 1, wv_b, slot, 1).wait()
    finish(pairs - 1, l_b, acc_b, wv_b, slot)

    third_done = min(max(turns - moe_at, 0), send_steps)
    last_done = min(max(turns - moe_at - 3, 0), send_steps)

    def third_rest(k, carry):
        third_step(k)
        return carry

    def last_rest(k, carry):
        last_step(k)
        return carry

    lax.fori_loop(third_done, send_steps, third_rest, 0)
    lax.fori_loop(last_done, send_steps, last_rest, 0)

    for d in range(zs - 1):

        @pl.when((z + 1 < zs) & (z - d >= 0))
        def _():
            for p in range(KV_PIECES):
                kv_send_to(z, x, c, partner, d, p).wait_send()

        @pl.when((z + 1 < zs) & (z - d >= 0))
        def _():
            tok_send_to(z, x, c, partner, 3 * zs + d).wait_send()

        @pl.when((z > 0) & (z + d < zs))
        def _():
            tok_send_to(z, x, c, partner, 4 * zs - 1 + d).wait_send()

    for d in range(zs):

        @pl.when(z - d >= 0)
        def _():
            for base in (zs - 1, 2 * zs - 1, 3 * zs - 1):
                for p in range(KV_PIECES):
                    kv_send_to(z, x, c, partner, base + d, p).wait_send()

    for index in range(3 * zs):
        tok_send_to(z, x, c, partner, index).wait_send()

    def drain(k, carry):
        first_copy(k).wait_send()
        second_copy(k).wait_send()
        for d in range(1, zs):
            third_copy(k, d).wait_send()
        return carry

    lax.fori_loop(0, send_steps, drain, 0)


def per_device(queries, latent_kv, w_value, moe_tokens, routes, router, w_gate, w_up, w_down):
    seq_dev, heads, width = queries.shape
    latent, vdim = w_value.shape[1], w_value.shape[2]
    scale = (vdim + width - latent) ** (-0.5)
    tb, top = routes.shape
    ep_size = lax.axis_size("ep")
    experts = router.shape[1]
    assert experts == ep_size and w_gate.shape[0] == 1 and ep_size % 4 == 0
    model, ff = moe_tokens.shape[1], w_gate.shape[2]
    cap = min(tb, 3 * tb * top // (2 * experts))
    zs = ep_size // 4
    wide = -(-width // LANES) * LANES
    keys = ep_size * seq_dev
    group, group_slots = ep_size * tb // 2, ep_size * cap // 2
    ufc = min(512, ff)
    dfc = min(1024, model)
    fc = min(512, model)
    send_steps = model // fc
    dims = (zs, heads, width, latent, vdim, seq_dev, tb, model, ff, experts, cap, scale, ufc, dfc,
            fc)
    cols = 2 * seq_dev
    vmem, dma = pltpu.VMEM, pltpu.SemaphoreType.DMA
    scratch = [
        vmem((zs, wide, 4 * seq_dev), BF16),
        vmem((keys, wide), BF16),
        vmem((2, wide, cols), BF16),
        vmem((2, wide, cols), BF16),
        vmem((keys, cols), F32),
        vmem((keys, cols), F32),
        vmem((8, cols), F32),
        vmem((8, cols), F32),
        vmem((8, cols), F32),
        vmem((8, cols), F32),
        vmem((latent, cols), F32),
        vmem((latent, cols), F32),
        vmem((2, 2, latent, vdim), BF16),
        vmem((2, 2, latent, vdim), BF16),
        vmem((2, group, model + LANES), BF16),
        vmem((LANES, LANES), F32),
        vmem((2 * group_slots, model), BF16),
        vmem((2 * group_slots, ff), BF16),
        vmem((2, group, group_slots), BF16),
        vmem((2, group, 1), F32),
        vmem((2, group, model), BF16),
        vmem((group, model), BF16),
        vmem((group, model), BF16),
        vmem((group // 2, model), BF16),
        vmem((group // 2, model), BF16),
        vmem((zs - 1, tb, model), BF16),
        vmem((UP_SLOTS, model, ufc), BF16),
        vmem((UP_SLOTS, model, ufc), BF16),
        vmem((DOWN_SLOTS, ff, dfc), BF16),
        dma((2, 2, 2)),
        dma((2, 2)),
        dma((2,)),
        dma((4 * zs - 1, KV_PIECES)),
        dma((4 * zs, KV_PIECES)),
        dma((5 * zs - 2,)),
        dma((4 * zs,)),
        dma((UP_SLOTS,)),
        dma((UP_SLOTS,)),
        dma((DOWN_SLOTS,)),
        dma((send_steps,)),
        dma((send_steps,)),
        dma((send_steps,)),
        dma((send_steps,)),
        dma((send_steps, zs - 1)),
        dma((send_steps, zs - 1)),
    ]
    hbm = pl.BlockSpec(memory_space=pl.ANY)
    local = pl.BlockSpec(memory_space=pltpu.VMEM)
    attention_out, moe_out = pl.pallas_call(
        functools.partial(layer_kernel, dims),
        in_specs=[hbm, hbm, hbm, hbm, local, local, hbm, hbm, hbm],
        out_specs=[local, local],
        out_shape=[
            jax.ShapeDtypeStruct((seq_dev, heads * vdim), BF16),
            jax.ShapeDtypeStruct((tb, model), BF16),
        ],
        scratch_shapes=scratch,
        compiler_params=pltpu.CompilerParams(
            vmem_limit_bytes=67043328, collective_id=0, has_side_effects=True
        ),
        cost_estimate=pl.CostEstimate(
            flops=heads * seq_dev * keys * (width + latent) * 2,
            bytes_accessed=6 * model * ff,
            transcendentals=heads * seq_dev * keys,
        ),
    )(
        jnp.transpose(queries, (1, 2, 0)),
        jnp.transpose(latent_kv),
        w_value,
        moe_tokens,
        jnp.transpose(routes),
        jnp.transpose(router),
        w_gate,
        w_up,
        w_down,
    )
    if lax.axis_size("node") > 1:
        moe_out = lax.psum_scatter(moe_out, "node", scatter_dimension=1, tiled=True)
    return (attention_out, moe_out)


def solution(mesh):
    placed = (
        P(("groups", "ep"), "node", None),
        P(("groups", "ep"), None),
        P("node", None, None),
        P(("groups", "ep"), None),
        P(("groups", "ep"), None),
        P(),
        P("ep", None, "node"),
        P("ep", None, "node"),
        P("ep", "node", None),
    )
    return jax.shard_map(
        per_device,
        mesh=mesh,
        in_specs=placed,
        out_specs=(P(("groups", "ep"), "node"), P(("groups", "ep"), "node")),
        check_vma=False,
    )
```
